128 devices in a mesh: seq: 64 (over z_hi, x, y, core), dp: 2 (over z_lo).
Axes of the slice: x: 4, y: 4, z: 4 (z_hi: 2, z_lo: 2; z = z_hi * 2 + z_lo), core: 2. Of those that a mesh axis runs over, the one named last changes fastest.
Arguments:
- block_pos: int32 [2, 128], P('dp'), may hold values from 0 to 127, as said below
- queries: bfloat16 [2, 8192, 2048], P('dp', 'seq'), may hold values from -8 to 8
- keys: bfloat16 [2, 8192, 2048], P('dp', 'seq'), may hold values from -4 to 4
- values: bfloat16 [2, 8192, 2048], P('dp', 'seq'), may hold values from -4 to 4
- attn_out: bfloat16 [2, 8192, 2048], P('dp', 'seq'), may hold values from -4 to 4, as said below
- log_sums: float32 [2, 16, 8192], P('dp', None, 'seq'), as said below
- grad_out: bfloat16 [2, 8192, 2048], P('dp', 'seq'), may hold values from -0.375 to 0.375
- out_weight: bfloat16 [2048, 2048], replicated, may hold values from -12 to 12
Outputs:
- grad_queries: bfloat16 [2, 8192, 2048], P('dp', 'seq')
- grad_keys: bfloat16 [2, 8192, 2048], P('dp', 'seq')
- grad_values: bfloat16 [2, 8192, 2048], P('dp', 'seq')
- grad_weight: float32 [2048, 2048], P('seq')
The draws below stay inside these ranges and needn't reach their ends.
Inputs may be any that keep to these rules, and one draw needn't show every extreme that they name: Each row is a permutation of 0 to 127; row block c (rows c * 64 to c * 64 + 63) holds the rows at positions block_pos[b, c] * 64 onward, in order. attn_out is the forward attention output: per head, exp(scores - log_sums) on the allowed keys times values, rounded to bfloat16. log_sums[b, h, t] is the log of the sum of exp(scores[b, h, t, u]) over the keys u with pos[b, u] <= pos[b, t].
All inputs are finite; a program needn't handle non-finite values.
Results may differ from the reference program's by a relative error of at most 0.0075.
Values may be sent and summed in bfloat16 or wider, within the bound.
No kernel may reach another device: no remote copies, remote signals or barrier semaphores. Data moves between devices by JAX's collectives and lax.ppermute only.
A program may use at most 320 MiB of HBM per device.

```python
import jax
import jax.numpy as jnp
from jax import lax

HEADS = 16
HEAD_DIM = 128
DW = 2048
TOK_DEV = 128
HD = 2048
BLOCK = 64
GRID = 8
NC = 128
LEN = 8192
SEQS = 2
N_SEQ = 64


def fold_key(base, number):
    return jax.random.fold_in(base, number)


def saved_forward(key):
    base = fold_key(key, 11)
    tables = []
    for index in range(SEQS):
        tables.append(jax.random.permutation(fold_key(base, 100 + index), NC).astype(jnp.int32))
    table_all = jnp.stack(tables)
    width_all = HEADS * HEAD_DIM
    shape = (SEQS, LEN, width_all)
    query_raw = 2.0 * jax.random.truncated_normal(fold_key(base, 1), -4.0, 4.0, shape, jnp.float32)
    key_raw = jax.random.truncated_normal(fold_key(base, 2), -4.0, 4.0, shape, jnp.float32)
    value_raw = jax.random.truncated_normal(fold_key(base, 3), -4.0, 4.0, shape, jnp.float32)
    query_all = query_raw.astype(jnp.bfloat16).astype(jnp.float32)
    key_all = key_raw.astype(jnp.bfloat16).astype(jnp.float32)
    value_all = value_raw.astype(jnp.bfloat16).astype(jnp.float32)
    scaling = HEAD_DIM ** (-0.5)
    outputs = []
    logs = []
    for index in range(SEQS):
        row_index = jnp.arange(LEN, dtype=jnp.int32)
        positions = tables[index][row_index // BLOCK] * BLOCK + row_index % BLOCK
        allowed = positions[None, :] <= positions[:, None]

        def head_forward(pack):
            query_h, key_h, value_h = pack
            scores = jnp.dot(query_h, key_h.T, precision=lax.Precision.HIGHEST) * scaling
            scores = jnp.where(allowed, scores, -1e+30)
            row_max = jnp.max(scores, axis=1)
            log_row = row_max + jnp.log(jnp.sum(jnp.exp(scores - row_max[:, None]), axis=1))
            weights = jnp.exp(scores - log_row[:, None])
            return (jnp.dot(weights, value_h, precision=lax.Precision.HIGHEST), log_row)

        def to_heads(array):
            return jnp.transpose(array.reshape(LEN, HEADS, HEAD_DIM), (1, 0, 2))
        heads_out, heads_log = lax.map(head_forward, (to_heads(query_all[index]), to_heads(key_all[index]), to_heads(value_all[index])))
        outputs.append(jnp.transpose(heads_out, (1, 0, 2)).reshape(LEN, width_all))
        logs.append(heads_log)
    return (table_all, query_all, key_all, value_all, jnp.stack(outputs), jnp.stack(logs))


def draw_block_pos(key, part):
    return saved_forward(key)[0].astype(jnp.int32)


def draw_queries(key, part):
    return saved_forward(key)[1].astype(jnp.bfloat16)


def draw_keys(key, part):
    return saved_forward(key)[2].astype(jnp.bfloat16)


def draw_values(key, part):
    return saved_forward(key)[3].astype(jnp.bfloat16)


def draw_attn_out(key, part):
    return saved_forward(key)[4].astype(jnp.bfloat16)


def draw_log_sums(key, part):
    return saved_forward(key)[5].astype(jnp.float32)


def levels(key, dims, split, low, high):
    def one(axis_at, blocks):
        steps = jax.random.uniform(jax.random.fold_in(jax.random.fold_in(key, 6), axis_at), (blocks,), jnp.float32, low / len(split), high / len(split))
        return jnp.repeat(jnp.exp(steps), dims[axis_at] // blocks).reshape((-1,) + (1,) * (len(dims) - axis_at - 1))

    loudness = one(*split[0])
    for cut in split[1:]:
        loudness = loudness * one(*cut)
    return loudness


def scatter_about(own_key, dims, width, reach, cuts=(), kind=jnp.bfloat16):
    entries = width * jax.random.normal(own_key, dims, jnp.float32)
    if cuts:
        entries = entries * levels(own_key, dims, cuts, -0.22, 0.18)
    return jnp.clip(entries, -reach, reach).astype(kind)


def setup_inputs(seed: int = 0) -> dict:
    seeds = jax.random.split(jax.random.key(seed), 9)
    block_pos = draw_block_pos(jax.random.fold_in(seeds[8], 71), 0)
    queries = draw_queries(jax.random.fold_in(seeds[8], 71), 0)
    keys = draw_keys(jax.random.fold_in(seeds[8], 71), 0)
    values = draw_values(jax.random.fold_in(seeds[8], 71), 0)
    attn_out = draw_attn_out(jax.random.fold_in(seeds[8], 71), 0)
    log_sums = draw_log_sums(jax.random.fold_in(seeds[8], 71), 0)
    grad_out = scatter_about(seeds[6], (SEQS, LEN, DW), 0.0625, 0.375, ((0, 2), (1, 64)))
    out_weight = scatter_about(seeds[7], (HD, DW), 2.0, 12.0)
    return dict(block_pos=block_pos, queries=queries, keys=keys, values=values, attn_out=attn_out, log_sums=log_sums, grad_out=grad_out, out_weight=out_weight)


def run_tables():
    query_owner = jnp.arange(N_SEQ, dtype=jnp.int32)[:, None]
    key_owner = jnp.arange(N_SEQ, dtype=jnp.int32)[None, :]
    distance = (query_owner - key_owner) % N_SEQ
    query_run = (-distance) % GRID
    key_run = ((distance + query_run) // GRID) % GRID
    choose = jnp.arange(GRID, dtype=jnp.int32)
    query_onehot = (query_run[:, :, None] == choose[None, None, :]).astype(jnp.float32)
    key_onehot = (key_run[:, :, None] == choose[None, None, :]).astype(jnp.float32)
    return query_onehot, key_onehot


def grouped_sum(pairs, runs, pattern):
    grouped = jnp.einsum(pattern, pairs, runs, precision=lax.Precision.HIGHEST)
    rounded = lax.optimization_barrier(grouped.astype(jnp.bfloat16))
    return jnp.sum(rounded.astype(jnp.float32), axis=1)


def one_sequence(table_row, query_rows, key_rows, value_rows, saved_out, log_rows, cotangent, out_weight, query_onehot, key_onehot):
    length = query_rows.shape[0]
    width_all = query_rows.shape[1]
    head_count = log_rows.shape[0]
    head_dim = width_all // head_count
    scaling = head_dim ** -0.5
    grad_heads = jnp.dot(cotangent, out_weight.T, preferred_element_type=jnp.float32).astype(jnp.bfloat16)
    deltas = jnp.sum((grad_heads.astype(jnp.float32) * saved_out.astype(jnp.float32)).reshape(length, head_count, head_dim), axis=-1).T
    row_index = jnp.arange(length, dtype=jnp.int32)
    positions = table_row[row_index // BLOCK] * BLOCK + row_index % BLOCK
    allowed = positions[None, :] <= positions[:, None]

    def to_heads(array):
        return jnp.transpose(array.reshape(length, head_count, head_dim), (1, 0, 2))

    def per_head(pack):
        query_h, key_h, value_h, grad_h, log_h, delta_h = pack
        scores = jnp.dot(query_h, key_h.T, preferred_element_type=jnp.float32) * scaling
        attn_probs = jnp.where(allowed, jnp.exp(scores - log_h[:, None]), 0.0)
        probs_low = lax.optimization_barrier(attn_probs.astype(jnp.bfloat16))
        dprobs = jnp.dot(grad_h, value_h.T, preferred_element_type=jnp.float32)
        dscores = attn_probs * (dprobs - delta_h[:, None])
        dscores_low = lax.optimization_barrier(dscores.astype(jnp.bfloat16))
        probs_four = probs_low.astype(jnp.float32).reshape(N_SEQ, TOK_DEV, N_SEQ, TOK_DEV)
        dscore_four = dscores_low.astype(jnp.float32).reshape(N_SEQ, TOK_DEV, N_SEQ, TOK_DEV)
        query_four = query_h.astype(jnp.float32).reshape(N_SEQ, TOK_DEV, head_dim)
        key_four = key_h.astype(jnp.float32).reshape(N_SEQ, TOK_DEV, head_dim)
        grad_four = grad_h.astype(jnp.float32).reshape(N_SEQ, TOK_DEV, head_dim)
        value_pairs = jnp.einsum("iajb,iac->ijbc", probs_four, grad_four, precision=lax.Precision.HIGHEST)
        value_grad = grouped_sum(value_pairs, key_onehot, "ijbc,ijt->jtbc")
        key_pairs = scaling * jnp.einsum("iajb,iac->ijbc", dscore_four, query_four, precision=lax.Precision.HIGHEST)
        key_grad = grouped_sum(key_pairs, key_onehot, "ijbc,ijt->jtbc")
        query_pairs = scaling * jnp.einsum("iajb,jbc->ijac", dscore_four, key_four, precision=lax.Precision.HIGHEST)
        query_grad = grouped_sum(query_pairs, query_onehot, "ijac,ijt->itac")
        return (query_grad.reshape(length, head_dim), key_grad.reshape(length, head_dim), value_grad.reshape(length, head_dim))

    packed = (to_heads(query_rows), to_heads(key_rows), to_heads(value_rows), to_heads(grad_heads), log_rows, deltas)
    query_grad, key_grad, value_grad = lax.map(per_head, packed)

    def from_heads(array):
        return jnp.transpose(array, (1, 0, 2)).reshape(length, width_all).astype(jnp.bfloat16)

    weight_grad = jnp.dot(saved_out.T, cotangent, preferred_element_type=jnp.float32)
    return from_heads(query_grad), from_heads(key_grad), from_heads(value_grad), weight_grad


def reference(block_pos, queries, keys, values, attn_out, log_sums, grad_out, out_weight):
    query_onehot, key_onehot = run_tables()
    query_list = []
    key_list = []
    value_list = []
    weight_total = jnp.zeros(out_weight.shape, jnp.float32)
    for index in range(SEQS):
        outcome = one_sequence(block_pos[index], queries[index], keys[index], values[index], attn_out[index], log_sums[index], grad_out[index], out_weight, query_onehot, key_onehot)
        query_list.append(outcome[0])
        key_list.append(outcome[1])
        value_list.append(outcome[2])
        weight_total = weight_total + outcome[3]
    return (jnp.stack(query_list), jnp.stack(key_list), jnp.stack(value_list), weight_total)
```

```python
import functools

import jax, jax.numpy as jnp
from jax import lax
from jax.experimental import pallas as pl
from jax.experimental.pallas import tpu as pltpu
from jax.sharding import Mesh
from jax.sharding import PartitionSpec as P

LOG2E = 1.4426950408889634


def attn_body(plan, q_rank, k_rank, k_base, q_pos, stats, qd_own, qd_far, kv_own, kv_far,
              dq_own, dq_far, dk_own, dv_own, dkv_far,
              qs, dos, ks, vs, dqs, dks, dvs, *, tq, tk, scaling, dq_form):
    rows = qd_own.shape[0] * 128
    half = rows // 64
    for side, ref in enumerate((qd_own, qd_far)):
        for j in range(half):
            at = pl.ds(pl.multiple_of(q_rank[side * half + j] * 64, 64), 64)
            lo = (j % 2) * 64
            qs[at, :] = ref[j // 2, lo : lo + 64, :]
            dos[at, :] = ref[j // 2, 128 + lo : 192 + lo, :]
    for side, ref in enumerate((kv_own, kv_far)):
        for j in range(half):
            at = pl.ds(pl.multiple_of(k_rank[side * half + j] * 64, 64), 64)
            lo = (j % 2) * 64
            ks[at, :] = ref[j // 2, lo : lo + 64, :]
            vs[at, :] = ref[j // 2, 128 + lo : 192 + lo, :]
    dqs[...] = jnp.zeros_like(dqs)
    n_q = 2 * rows // tq
    n_k = 2 * rows // tk

    def k_step(i, _):
        k_at = pl.ds(pl.multiple_of(i * tk, tk), tk)
        dks[k_at, :] = jnp.zeros((tk, 128), jnp.float32)
        dvs[k_at, :] = jnp.zeros((tk, 128), jnp.float32)

        def tile(j, masked):
            q_at = pl.ds(pl.multiple_of(j * tq, tq), tq)
            k = ks[k_at, :]
            q = qs[q_at, :]
            do = dos[q_at, :]
            nt = (((1,), (1,)), ((), ()))
            s = lax.dot_general(k, q, nt, preferred_element_type=jnp.float32)
            p = jnp.exp2(s * (scaling * LOG2E) - stats[0:1, q_at])
            if masked:
                pos = q_pos[0:1, q_at]
                parts = []
                for b in range(tk // 64):
                    at = k_base[i * (tk // 64) + b] * 64 + lax.broadcasted_iota(jnp.int32, (64, tq), 0)
                    parts.append(jnp.where(at <= pos, p[b * 64 : b * 64 + 64], 0.0))
                p = jnp.concatenate(parts, axis=0)
            dvs[k_at, :] += jnp.dot(p.astype(jnp.bfloat16), do, preferred_element_type=jnp.float32)
            dp = lax.dot_general(vs[k_at, :], do, nt, preferred_element_type=jnp.float32)
            ds = (p * (dp - stats[1:2, q_at])).astype(jnp.bfloat16)
            dks[k_at, :] += jnp.dot(ds, q, preferred_element_type=jnp.float32)
            dqs[q_at, :] += lax.dot_general(ds, k, (((0,), (0,)), ((), ())), preferred_element_type=jnp.float32)
            return 0

        lax.fori_loop(plan[0, i], plan[1, i], lambda j, c: tile(j, True), 0)
        lax.fori_loop(plan[1, i], n_q, lambda j, c: tile(j, False), 0)
        return 0

    lax.fori_loop(0, n_k, k_step, 0)
    for j in range(half):
        own = pl.ds(pl.multiple_of(q_rank[j] * 64, 64), 64)
        far = pl.ds(pl.multiple_of(q_rank[half + j] * 64, 64), 64)
        lo = (j % 2) * 64
        dq_own[j // 2, lo : lo + 64, :] = dqs[own, :] * scaling
        dq_far[j // 2, lo : lo + 64, :] = (dqs[far, :] * scaling).astype(jnp.bfloat16)
        own = pl.ds(pl.multiple_of(k_rank[j] * 64, 64), 64)
        far = pl.ds(pl.multiple_of(k_rank[half + j] * 64, 64), 64)
        dk_own[j // 2, lo : lo + 64, :] = dks[own, :] * scaling
        dv_own[j // 2, lo : lo + 64, :] = dvs[own, :]
        dkv_far[j // 2, lo : lo + 64, :] = (dks[far, :] * scaling).astype(jnp.bfloat16)
        dkv_far[j // 2, 128 + lo : 192 + lo, :] = dvs[far, :].astype(jnp.bfloat16)


def attn(plan, q_rank, k_rank, k_base, q_pos, stats, qd_own, qd_far, kv_own, kv_far, *, tq, tk, scaling, dq_form=0):
    n = qd_own.shape[0]
    rows = 2 * n * 128
    smem = pl.BlockSpec(memory_space=pltpu.SMEM)
    vmem = pl.BlockSpec(memory_space=pltpu.VMEM)
    f32, bf = jnp.float32, jnp.bfloat16
    return pl.pallas_call(
        functools.partial(attn_body, tq=tq, tk=tk, scaling=scaling, dq_form=dq_form),
        in_specs=[smem] * 4 + [vmem] * 6,
        out_specs=[vmem] * 5,
        out_shape=[
            jax.ShapeDtypeStruct((n, 128, 128), f32),
            jax.ShapeDtypeStruct((n, 128, 128), bf),
            jax.ShapeDtypeStruct((n, 128, 128), f32),
            jax.ShapeDtypeStruct((n, 128, 128), f32),
            jax.ShapeDtypeStruct((n, 256, 128), bf),
        ],
        scratch_shapes=[pltpu.VMEM((rows, 128), bf)] * 4 + [pltpu.VMEM((rows, 128), f32)] * 3,
        compiler_params=pltpu.CompilerParams(vmem_limit_bytes=58 * 2**20),
        cost_estimate=pl.CostEstimate(flops=14 * 10**9, bytes_accessed=12 * 2**20, transcendentals=10**7),
        name="attn_grads",
    )(plan, q_rank, k_rank, k_base, q_pos, stats, qd_own, qd_far, kv_own, kv_far)


def tables(q_blocks, k_blocks, tq, tk):
    def ranked(b):
        rank = jnp.sum((b[:, None] > b[None, :]).astype(jnp.int32), axis=1)
        hot = rank[None, :] == jnp.arange(b.shape[0], dtype=jnp.int32)[:, None]
        return rank, hot, jnp.sum(jnp.where(hot, b[None, :], 0), axis=1)
    q_rank, q_hot, q_sorted = ranked(q_blocks)
    k_rank, k_hot, k_sorted = ranked(k_blocks)
    q_max = q_sorted[tq // 64 - 1 :: tq // 64]
    q_min = q_sorted[:: tq // 64]
    k_min = k_sorted[:: tk // 64]
    k_max = k_sorted[tk // 64 - 1 :: tk // 64]
    first = jnp.sum((q_max[None, :] < k_min[:, None]).astype(jnp.int32), axis=1)
    whole = jnp.sum((q_min[None, :] <= k_max[:, None]).astype(jnp.int32), axis=1)
    plan = jnp.stack([first, jnp.maximum(first, whole)])
    q_pos = (q_sorted[:, None] * 64 + jnp.arange(64, dtype=jnp.int32)[None, :]).reshape(1, -1)
    return plan, q_rank, k_rank, k_sorted, q_hot, q_pos


SEQ = ("z", "x", "y", "c")
F32, BF16 = jnp.float32, jnp.bfloat16
TQ, TK = 512, 512


def ring(array, axis, by):
    count = lax.axis_size(axis)
    return lax.ppermute(array, axis, [(i, (i + by) % count) for i in range(count)])


def pick(array, index, axis):
    return lax.dynamic_index_in_dim(array, index, axis, keepdims=False)


def pieces(rows):
    hi = lax.reduce_precision(rows, 8, 7)
    rest = rows - hi
    mid = lax.reduce_precision(rest, 8, 7)
    return [part.astype(BF16) for part in (hi, mid, rest - mid)]


def by_head(array):
    return jnp.transpose(array.reshape(128, 16, 128), (1, 0, 2))


def by_token(array):
    return jnp.transpose(array, (1, 0, 2)).reshape(128, 2048)


def weight_gather(saved, cotangent):
    x, y = lax.axis_index("x"), lax.axis_index("y")
    cols = saved.reshape(128, 2, 4, 256)
    own_cols = [pick(cols, (x + s) % 4, 2).reshape(128, 512) for s in range(4)]
    saved_parts = [own_cols[0]] + [ring(own_cols[s], "x", s) for s in range(1, 4)]
    outs = cotangent.reshape(128, 4, 512)
    own_outs = [pick(outs, (y + s) % 4, 1) for s in range(4)]
    cot_parts = [own_outs[0]] + [ring(own_outs[s], "y", s) for s in range(1, 4)]
    saved_own = jnp.stack(saved_parts)
    cot_own = jnp.stack(cot_parts)
    saved_all = [saved_own] + [ring(saved_own, "y", s) for s in range(1, 4)]
    cot_all = [cot_own] + [ring(cot_own, "x", s) for s in range(1, 4)]
    return saved_all, cot_all


def weight_grad(saved_all, cot_all):
    c = lax.axis_index("c")
    saved_rows = jnp.stack(saved_all).reshape(2048, 512)
    cot_rows = jnp.stack(cot_all, axis=1).reshape(2048, 512)
    block = lax.dot_general(saved_rows, cot_rows, (((0,), (0,)), ((), ())), preferred_element_type=F32)
    block = block.reshape(2, 4, 2, 32, 512)
    other = ring(pick(block, 1 - c, 2).astype(BF16), "c", 1)
    block = pick(block, c, 2) + other.astype(F32)
    sent = jnp.broadcast_to(block.astype(BF16)[:, None], (2, 2, 4, 32, 512)).reshape(16, 32, 512)
    got = lax.all_to_all(sent, ("z", "d", "y"), 0, 0, tiled=True)
    total = jnp.sum(got.reshape(4, 4, 32, 512).astype(F32), axis=0)
    return jnp.transpose(total, (1, 0, 2)).reshape(32, 2048)


def per_device(block_pos, queries, keys, values, attn_out, log_sums, grad_out, out_weight):
    z, c = lax.axis_index("z"), lax.axis_index("c")
    scaling = 128**-0.5
    cotangent, saved = grad_out[0], attn_out[0]
    heads = lax.dot_general(
        cotangent, out_weight, (((1,), (1,)), ((), ())), preferred_element_type=F32
    ).astype(BF16)
    delta = jnp.sum(
        (heads.astype(F32) * saved.astype(F32)).reshape(128, 16, 128), axis=-1
    ).T
    stats = pieces(log_sums[0]) + pieces(delta)
    stats = jnp.pad(jnp.stack(stats, axis=1), ((0, 0), (0, 10), (0, 0)))
    qd = jnp.concatenate([by_head(queries[0]), by_head(heads), stats], axis=1)
    kv = jnp.concatenate([by_head(keys[0]), by_head(values[0])], axis=1)
    qd_own = lax.all_to_all(qd, ("x", "y"), 0, 0, tiled=True)
    qd_far = ring(qd_own, "z", 1)
    kv_own = lax.all_to_all(kv, ("x", "y"), 0, 0, tiled=True)
    kv_far = ring(kv_own, "c", 1)
    saved_all, cot_all = weight_gather(saved, cotangent)

    where = block_pos[0].reshape(2, 16, 2, 2)
    q_blocks = pick(where, c, 2)
    q_blocks = jnp.concatenate([pick(q_blocks, z, 0).reshape(-1), pick(q_blocks, 1 - z, 0).reshape(-1)])
    k_blocks = pick(where, z, 0)
    k_blocks = jnp.concatenate([pick(k_blocks, c, 1).reshape(-1), pick(k_blocks, 1 - c, 1).reshape(-1)])
    plan, q_rank, k_rank, k_base, q_hot, q_pos = tables(q_blocks, k_blocks, TQ, TK)
    raw = jnp.concatenate([qd_own[:, 256:262], qd_far[:, 256:262]]).astype(F32).reshape(32, 2, 3, 2, 64)
    raw = jnp.transpose(jnp.sum(raw, axis=2), (1, 0, 2, 3)).reshape(2, 64, 64)
    rows = jnp.sum(jnp.where(q_hot[None, :, :, None], raw[:, None], 0.0), axis=2).reshape(2, -1)
    rows = jnp.concatenate([rows[:1] * LOG2E, rows[1:]])
    dq_own, dq_far, dk_own, dv_own, dkv_far = attn(
        plan, q_rank, k_rank, k_base, q_pos, rows, qd_own, qd_far, kv_own, kv_far,
        tq=TQ, tk=TK, scaling=scaling,
    )
    dq_got = ring(dq_far, "z", 1)
    dkv_got = ring(dkv_far, "c", 1).astype(F32)
    dkv = jnp.concatenate(
        [(dk_own + dkv_got[:, :128]).astype(BF16), (dv_own + dkv_got[:, 128:]).astype(BF16)], axis=1
    )
    dkv = lax.all_to_all(dkv, ("x", "y"), 0, 0, tiled=True)
    dq = (dq_own + dq_got.astype(F32)).astype(BF16)
    dq = lax.all_to_all(dq, ("x", "y"), 0, 0, tiled=True)
    return (
        by_token(dq)[None],
        by_token(dkv[:, :128])[None],
        by_token(dkv[:, 128:])[None],
        weight_grad(saved_all, cot_all),
    )


def solution(mesh):
    split = Mesh(mesh.devices.reshape(2, 4, 4, 2, 2), ("z", "x", "y", "c", "d"))
    rows = P("d", SEQ, None)
    return jax.shard_map(
        per_device,
        mesh=split,
        in_specs=(P("d", None), rows, rows, rows, rows, P("d", None, SEQ), rows, P()),
        out_specs=(rows, rows, rows, P(SEQ, None)),
        check_vma=False,
    )
```

```python
import functools

import jax
import jax.numpy as jnp
from jax import lax
from jax.experimental import pallas as pl
from jax.experimental.pallas import tpu as pltpu
from jax.sharding import Mesh
from jax.sharding import PartitionSpec as P

F32, BF16 = jnp.float32, jnp.bfloat16
LOG2E = 1.4426950408889634
NT = (((1,), (1,)), ((), ()))
TN = (((0,), (0,)), ((), ()))
SMEM = pl.BlockSpec(memory_space=pltpu.SMEM)
VMEM = pl.BlockSpec(memory_space=pltpu.VMEM)
HBM = pl.BlockSpec(memory_space=pltpu.HBM)


def like(shape, dtype):
    return jax.ShapeDtypeStruct(shape, dtype)


def pieces(row):
    hi = row.astype(BF16).astype(F32)
    mid = (row - hi).astype(BF16).astype(F32)
    return [hi, mid, row - hi - mid]


def first_body(side, queries, keys, values, saved, cot, packed, part0, part1, part2, part3):
    step = pl.program_id(0)
    for a in range(PACK):
        at = slice(a * 128, a * 128 + 128)
        packed[a, 0:128, :] = queries[:, at]
        packed[a, 128:256, :] = keys[:, at]
        packed[a, 256:384, :] = values[:, at]
    for s, part in enumerate((part0, part1, part2, part3)):
        target = (side[0] + s) % 4

        @pl.when(target // 2 == step)
        def _():
            part[:, 0:1024] = saved[...]

        @pl.when(target % 2 == step)
        def _():
            part[:, 1024:2048] = cot[...]


def second_body(cot, weight, saved, logs, packed):
    step = pl.program_id(0)
    heads = lax.dot_general(cot[...], weight[...], NT, preferred_element_type=F32).astype(BF16)
    delta = heads.astype(F32) * saved[...].astype(F32)
    row_id = lax.broadcasted_iota(jnp.int32, (16, 128), 0)
    for a in range(PACK):
        at = slice(a * 128, a * 128 + 128)
        row = jnp.sum(jnp.transpose(delta[:, at]), axis=0, keepdims=True)
        stats = jnp.zeros((16, 128), F32)
        for i, piece in enumerate(pieces(logs[pl.ds(step * PACK + a, 1), :] * LOG2E) + pieces(row)):
            stats = jnp.where(row_id == i, piece, stats)
        packed[a, 0:128, :] = heads[:, at]
        packed[a, 128:144, :] = stats.astype(BF16)


PACK = 8
WHOLE = pl.BlockSpec((128, 2048), lambda h: (0, 0))
COLUMNS = pl.BlockSpec((128, 128 * PACK), lambda h: (0, h))


def pack_first(side, queries, keys, values, saved, cot):
    return pl.pallas_call(
        first_body,
        grid=(16 // PACK,),
        in_specs=[SMEM] + [COLUMNS] * 5,
        out_specs=[pl.BlockSpec((PACK, 384, 128), lambda h: (h, 0, 0))] + [WHOLE] * 4,
        out_shape=[like((16, 384, 128), BF16)] + [like((128, 2048), BF16)] * 4,
        compiler_params=pltpu.CompilerParams(vmem_limit_bytes=60 * 2**20),
        name="pack_first",
    )(side, queries, keys, values, saved, cot)


def pack_second(cot, weight, saved, logs):
    return pl.pallas_call(
        second_body,
        grid=(16 // PACK,),
        in_specs=[WHOLE, pl.BlockSpec((128 * PACK, 2048), lambda h: (h, 0)), COLUMNS,
                  pl.BlockSpec((16, 128), lambda h: (0, 0))],
        out_specs=pl.BlockSpec((PACK, 144, 128), lambda h: (h, 0, 0)),
        out_shape=like((16, 144, 128), BF16),
        compiler_params=pltpu.CompilerParams(vmem_limit_bytes=40 * 2**20),
        name="pack_second",
    )(cot, weight, saved, logs)


def sort_rows(rank, base, count, pairs):
    for j in range(count):
        at = pl.ds(pl.multiple_of(rank[base + j] * 64, 64), 64)
        for src, lo, dst in pairs:
            lo += (j % 2) * 64
            dst[at, :] = src[j // 2, lo : lo + 64, :]


def place_stats(q_rank, qd, stats_s):
    low = lax.broadcasted_iota(jnp.int32, (1, 128), 1) < 64
    for j in range(16):
        raw = qd[j, 128:144, :].astype(F32)
        for kind in range(2):
            row = raw[3 * kind : 3 * kind + 1] + raw[3 * kind + 1 : 3 * kind + 2] + raw[3 * kind + 2 : 3 * kind + 3]
            turned = pltpu.roll(row, 64, 1)
            for sub in range(2):
                r = q_rank[2 * j + sub]
                upper = r % 2
                value = jnp.where(upper == sub, row, turned)
                at = pl.ds(r // 2, 1)
                keep = jnp.logical_xor(low, upper == 1)
                stats_s[kind, at, :] = jnp.where(keep, value, stats_s[kind, at, :])


def tiles(plan, q_base, k_base, qs, dos, ks, vs, stats_s, dqs, dks, dvs, tq, tk, scaling, start, finish):
    n_q = qs.shape[0] // tq
    n_k = ks.shape[0] // tk
    lane = lax.broadcasted_iota(jnp.int32, (1, 128), 1)

    def k_step(i, _):
        k_at = pl.ds(pl.multiple_of(i * tk, tk), tk)
        start(i, k_at)

        def tile(j, masked):
            q_at = pl.ds(pl.multiple_of(j * tq, tq), tq)
            spans = range(tq // 128)
            logs = jnp.concatenate([stats_s[0, pl.ds(j * (tq // 128) + a, 1), :] for a in spans], axis=1)
            delta = jnp.concatenate([stats_s[1, pl.ds(j * (tq // 128) + a, 1), :] for a in spans], axis=1)
            k = ks[k_at, :]
            q = qs[q_at, :]
            do = dos[q_at, :]
            s = lax.dot_general(k, q, NT, preferred_element_type=F32)
            p = jnp.exp2(s * (scaling * LOG2E) - logs)
            if masked:
                pos = []
                for a in spans:
                    b = (j * (tq // 128) + a) * 2
                    pos.append(jnp.where(lane < 64, q_base[b] * 64 + lane, q_base[b + 1] * 64 + lane - 64))
                pos = jnp.concatenate(pos, axis=1)
                parts = []
                for b in range(tk // 64):
                    at = k_base[i * (tk // 64) + b] * 64 + lax.broadcasted_iota(jnp.int32, (64, tq), 0)
                    parts.append(jnp.where(at <= pos, p[b * 64 : b * 64 + 64], 0.0))
                p = jnp.concatenate(parts, axis=0)
            dvs[k_at, :] += jnp.dot(p.astype(BF16), do, preferred_element_type=F32)
            dp = lax.dot_general(vs[k_at, :], do, NT, preferred_element_type=F32)
            ds = (p * (dp - delta)).astype(BF16)
            dks[k_at, :] += jnp.dot(ds, q, preferred_element_type=F32)
            dqs[q_at, :] += lax.dot_general(ds, k, TN, preferred_element_type=F32)
            return 0

        lax.fori_loop(plan[0, i], plan[1, i], lambda j, c: tile(j, True), 0)
        lax.fori_loop(plan[1, i], n_q, lambda j, c: tile(j, False), 0)
        finish(i, k_at)
        return 0

    lax.fori_loop(0, n_k, k_step, 0)


def near_body(plan, q_rank, q_base, k_rank, k_base, own, grads, kv_far, dq, dk_out, dv_out,
              qs, dos, ks, vs, stats_s, dqs, dks, dvs, sems, kv_s, fetch_sem, *, tq, tk, scaling):
    fetch = pltpu.make_async_copy(kv_far, kv_s, fetch_sem)
    fetch.start()
    sort_rows(q_rank, 0, 32, [(own, 0, qs), (grads, 0, dos)])
    sort_rows(k_rank, 0, 32, [(own, 128, ks), (own, 256, vs)])
    place_stats(q_rank, grads, stats_s)
    fetch.wait()
    sort_rows(k_rank, 32, 32, [(kv_s, 0, ks), (kv_s, 128, vs)])
    dqs[...] = jnp.zeros_like(dqs)

    def copies(i, k_at):
        return (
            pltpu.make_async_copy(dks.at[k_at, :], dk_out.at[k_at, :], sems.at[0, i]),
            pltpu.make_async_copy(dvs.at[k_at, :], dv_out.at[k_at, :], sems.at[1, i]),
        )

    def start(i, k_at):
        dks[k_at, :] = jnp.zeros((tk, 128), F32)
        dvs[k_at, :] = jnp.zeros((tk, 128), F32)

    def finish(i, k_at):
        for copy in copies(i, k_at):
            copy.start()

    tiles(plan, q_base, k_base, qs, dos, ks, vs, stats_s, dqs, dks, dvs, tq, tk, scaling, start, finish)
    for i in range(4096 // tk):
        for copy in copies(i, pl.ds(i * tk, tk)):
            copy.wait()
    for j in range(32):
        at = pl.ds(pl.multiple_of(q_rank[j] * 64, 64), 64)
        lo = (j % 2) * 64
        dq[j // 2, lo : lo + 64, :] = dqs[at, :] * scaling


def far_body(plan, q_rank, q_base, k_rank, k_base, own, kv_far, q_far, grads, dk_in, dv_in,
             dq_far, dk_own, dv_own, dkv_far,
             qs, dos, ks, vs, stats_s, dqs, dks, dvs, sems, kv_s, fetch_sem, *, tq, tk, scaling):
    def copies(i, k_at):
        return (
            pltpu.make_async_copy(dk_in.at[k_at, :], dks.at[k_at, :], sems.at[0, i]),
            pltpu.make_async_copy(dv_in.at[k_at, :], dvs.at[k_at, :], sems.at[1, i]),
        )

    for i in range(4096 // tk):
        for copy in copies(i, pl.ds(i * tk, tk)):
            copy.start()
    fetch = pltpu.make_async_copy(kv_far, kv_s, fetch_sem)
    fetch.start()
    sort_rows(q_rank, 0, 32, [(q_far, 0, qs), (grads, 0, dos)])
    sort_rows(k_rank, 0, 32, [(own, 128, ks), (own, 256, vs)])
    place_stats(q_rank, grads, stats_s)
    fetch.wait()
    sort_rows(k_rank, 32, 32, [(kv_s, 0, ks), (kv_s, 128, vs)])
    dqs[...] = jnp.zeros_like(dqs)

    def start(i, k_at):
        for copy in copies(i, k_at):
            copy.wait()

    def finish(i, k_at):
        pass

    tiles(plan, q_base, k_base, qs, dos, ks, vs, stats_s, dqs, dks, dvs, tq, tk, scaling, start, finish)
    for j in range(32):
        at = pl.ds(pl.multiple_of(q_rank[j] * 64, 64), 64)
        own_at = pl.ds(pl.multiple_of(k_rank[j] * 64, 64), 64)
        far_at = pl.ds(pl.multiple_of(k_rank[32 + j] * 64, 64), 64)
        lo = (j % 2) * 64
        dq_far[j // 2, lo : lo + 64, :] = (dqs[at, :] * scaling).astype(BF16)
        dk_own[j // 2, lo : lo + 64, :] = dks[own_at, :] * scaling
        dv_own[j // 2, lo : lo + 64, :] = dvs[own_at, :]
        dkv_far[j // 2, lo : lo + 64, :] = (dks[far_at, :] * scaling).astype(BF16)
        dkv_far[j // 2, 128 + lo : 192 + lo, :] = dvs[far_at, :].astype(BF16)


COST = pl.CostEstimate(flops=7 * 10**9, bytes_accessed=12 * 2**20, transcendentals=10**7)
SORTED = [pltpu.VMEM((2048, 128), BF16)] * 2 + [pltpu.VMEM((4096, 128), BF16)] * 2
SORTED += [pltpu.VMEM((2, 16, 128), F32), pltpu.VMEM((2048, 128), F32)]
FETCH = [pltpu.VMEM((16, 256, 128), BF16), pltpu.SemaphoreType.DMA]
TOTALS = [pltpu.VMEM((4096, 128), F32)] * 2


def in_hbm(array):
    return pltpu.with_memory_space_constraint(array, pltpu.HBM)


def attn_near(tables, own, grads, kv_far, tq, tk, scaling):
    return pl.pallas_call(
        functools.partial(near_body, tq=tq, tk=tk, scaling=scaling),
        in_specs=[SMEM] * 5 + [VMEM] * 2 + [HBM],
        out_specs=[VMEM, HBM, HBM],
        out_shape=[like((16, 128, 128), F32)] + [pltpu.HBM((4096, 128), F32)] * 2,
        scratch_shapes=SORTED + TOTALS + [pltpu.SemaphoreType.DMA((2, 4096 // tk))] + FETCH,
        compiler_params=pltpu.CompilerParams(vmem_limit_bytes=28 * 2**20),
        cost_estimate=COST,
        name="attn_near",
    )(*tables, own, grads, in_hbm(kv_far))


def attn_far(tables, own, kv_far, q_far, grads, dk_in, dv_in, tq, tk, scaling):
    return pl.pallas_call(
        functools.partial(far_body, tq=tq, tk=tk, scaling=scaling),
        in_specs=[SMEM] * 5 + [VMEM, HBM, VMEM, VMEM] + [HBM] * 2,
        out_specs=[VMEM] * 4,
        out_shape=[like((16, 128, 128), BF16), like((16, 128, 128), F32), like((16, 128, 128), F32),
                   like((16, 256, 128), BF16)],
        scratch_shapes=SORTED + TOTALS + [pltpu.SemaphoreType.DMA((2, 4096 // tk))] + FETCH,
        compiler_params=pltpu.CompilerParams(vmem_limit_bytes=28 * 2**20),
        cost_estimate=COST,
        name="attn_far",
    )(*tables, own, in_hbm(kv_far), q_far, grads, in_hbm(dk_in), in_hbm(dv_in))


def ranked(blocks):
    rank = jnp.sum((blocks[:, None] > blocks[None, :]).astype(jnp.int32), axis=1)
    hot = rank[None, :] == jnp.arange(blocks.shape[0], dtype=jnp.int32)[:, None]
    return rank, jnp.sum(jnp.where(hot, blocks[None, :], 0), axis=1)


def make_plan(q_sorted, k_sorted, tq, tk):
    q_max = q_sorted[tq // 64 - 1 :: tq // 64]
    q_min = q_sorted[:: tq // 64]
    k_min = k_sorted[:: tk // 64]
    k_max = k_sorted[tk // 64 - 1 :: tk // 64]
    first = jnp.sum((q_max[None, :] < k_min[:, None]).astype(jnp.int32), axis=1)
    whole = jnp.sum((q_min[None, :] <= k_max[:, None]).astype(jnp.int32), axis=1)
    return jnp.stack([first, jnp.maximum(first, whole)])


def weight_body(side, part0, part1, part2, part3, kept, given, total):
    parts = [part[...] for part in (part0, part1, part2, part3)]
    rows = jnp.concatenate([part[:, :1024] for part in parts], axis=0)
    cols = jnp.concatenate([part[:, 1024:] for part in parts], axis=0)
    total[...] = lax.dot_general(rows, cols, TN, preferred_element_type=F32)
    c = side[0]
    for block in range(16):
        mine = pl.ds(pl.multiple_of((block * 2 + c) * 32, 32), 32)
        other = pl.ds(pl.multiple_of((block * 2 + 1 - c) * 32, 32), 32)
        kept[block, :, :] = total[mine, :]
        given[block, :, :] = total[other, :].astype(BF16)


def weight_block(side, parts):
    return pl.pallas_call(
        weight_body,
        grid=(1,),
        in_specs=[SMEM] + [pl.BlockSpec((128, 2048), lambda i: (0, 0))] * 4,
        out_specs=[pl.BlockSpec((16, 32, 1024), lambda i: (0, 0, 0))] * 2,
        out_shape=[pltpu.HBM((16, 32, 1024), F32), like((16, 32, 1024), BF16)],
        scratch_shapes=[pltpu.VMEM((1024, 1024), F32)],
        compiler_params=pltpu.CompilerParams(vmem_limit_bytes=28 * 2**20),
        cost_estimate=pl.CostEstimate(flops=2 * 10**9, bytes_accessed=6 * 2**20, transcendentals=0),
        name="weight_block",
    )(side, *parts)


SEQ = ("z", "x", "y", "c")
TQ, TK = 512, 1024


def ring(array, axis, by):
    count = lax.axis_size(axis)
    return lax.ppermute(array, axis, [(i, (i + by) % count) for i in range(count)])


def pick(array, index, axis):
    return lax.dynamic_index_in_dim(array, index, axis, keepdims=False)


def by_token(array):
    return jnp.transpose(array, (1, 0, 2)).reshape(1, 128, 2048)


def step(block_pos, queries, keys, values, attn_out, log_sums, grad_out, out_weight):
    z, c, d = lax.axis_index("z"), lax.axis_index("c"), lax.axis_index("d")
    scaling = 128**-0.5
    packed, *parts = pack_first((z * 2 + d).reshape(1), queries[0], keys[0], values[0], attn_out[0], grad_out[0])
    own = lax.all_to_all(packed, ("x", "y"), 0, 0, tiled=True)
    parts = parts[:1] + [ring(parts[s], ("z", "d"), s) for s in range(1, 4)]
    packed = pack_second(grad_out[0], out_weight, attn_out[0], log_sums[0])
    grads = lax.all_to_all(packed, ("x", "y"), 0, 0, tiled=True)

    where = block_pos[0].reshape(2, 16, 2, 2)
    q_blocks = pick(where, c, 2)
    k_blocks = pick(where, z, 0)
    k_blocks = jnp.concatenate([pick(k_blocks, c, 1).reshape(-1), pick(k_blocks, 1 - c, 1).reshape(-1)])
    k_rank, k_sorted = ranked(k_blocks)
    tables = []
    for side in (z, 1 - z):
        q_rank, q_sorted = ranked(pick(q_blocks, side, 0).reshape(-1))
        tables.append((make_plan(q_sorted, k_sorted, TQ, TK), q_rank, q_sorted, k_rank, k_sorted))

    kept, given = weight_block(c.reshape(1), parts)
    given = ring(given, "c", 1)
    grads, tables = lax.optimization_barrier((grads, tables))
    kv_far = ring(own[:, 128:], "c", 1)
    q_far = ring(own[:, :128], "z", 1)
    grads_far = ring(grads, "z", 1)
    dq_near, dk_near, dv_near = attn_near(tables[0], own, grads, kv_far, TQ, TK, scaling)
    dk_near, kept, given = lax.optimization_barrier((dk_near, kept, given))
    blocks = (kept + given.astype(F32)).astype(BF16)
    blocks = lax.all_to_all(blocks, ("x", "y"), 0, 0, tiled=True)
    dq_far, dk_own, dv_own, dkv_far = attn_far(
        tables[1], own, kv_far, q_far, grads_far, dk_near, dv_near, TQ, TK, scaling
    )
    dkv_got = ring(dkv_far, "c", 1).astype(F32)
    dq_got = ring(dq_far, "z", 1)
    dkv = jnp.concatenate(
        [(dk_own + dkv_got[:, :128]).astype(BF16), (dv_own + dkv_got[:, 128:]).astype(BF16)], axis=1
    )
    dkv_out = lax.all_to_all(dkv, ("x", "y"), 0, 0, tiled=True)
    blocks, _ = lax.optimization_barrier((blocks, dkv))
    mine = jnp.sum(blocks.astype(F32), axis=0)
    other = ring(mine, "d", 1)
    weight = jnp.where(d == 0, jnp.concatenate([mine, other], axis=1), jnp.concatenate([other, mine], axis=1))

    dq_near, dq_got, _ = lax.optimization_barrier((dq_near, dq_got, dkv))
    dq = (dq_near + dq_got.astype(F32)).astype(BF16)
    dq, dkv_out = lax.optimization_barrier((dq, dkv_out))
    dq_out = lax.all_to_all(dq, ("x", "y"), 0, 0, tiled=True)
    return by_token(dq_out), by_token(dkv_out[:, :128]), by_token(dkv_out[:, 128:]), weight


def solution(mesh):
    split = Mesh(mesh.devices.reshape(2, 4, 4, 2, 2), ("z", "x", "y", "c", "d"))
    rows = P("d", SEQ, None)
    return jax.shard_map(
        step,
        mesh=split,
        in_specs=(P("d", None), rows, rows, rows, rows, P("d", None, SEQ), rows, P()),
        out_specs=(rows, rows, rows, P(SEQ, None)),
        check_vma=False,
    )
```

```python
import functools

import jax
import jax.numpy as jnp
from jax import lax
from jax.experimental import pallas as pl
from jax.experimental.pallas import tpu as pltpu
from jax.sharding import Mesh
from jax.sharding import PartitionSpec as P

F32, BF16 = jnp.float32, jnp.bfloat16
LOG2E = 1.4426950408889634
NT = (((1,), (1,)), ((), ()))
TN = (((0,), (0,)), ((), ()))
SMEM = pl.BlockSpec(memory_space=pltpu.SMEM)
VMEM = pl.BlockSpec(memory_space=pltpu.VMEM)
HBM = pl.BlockSpec(memory_space=pltpu.HBM)


def like(shape, dtype):
    return jax.ShapeDtypeStruct(shape, dtype)


def pieces(row):
    hi = row.astype(BF16).astype(F32)
    mid = (row - hi).astype(BF16).astype(F32)
    return [hi, mid, row - hi - mid]


def first_body(side, queries, keys, values, saved, cot, packed, part0, part1, part2, part3):
    step = pl.program_id(0)
    for a in range(PACK):
        at = slice(a * 128, a * 128 + 128)
        packed[a, 0:128, :] = queries[:, at]
        packed[a, 128:256, :] = keys[:, at]
        packed[a, 256:384, :] = values[:, at]
    for s, part in enumerate((part0, part1, part2, part3)):
        target = (side[0] + s) % 4

        @pl.when(target // 2 == step)
        def _():
            part[:, 0:1024] = saved[...]

        @pl.when(target % 2 == step)
        def _():
            part[:, 1024:2048] = cot[...]


def second_body(cot, weight, saved, logs, packed):
    step = pl.program_id(0)
    heads = lax.dot_general(cot[...], weight[...], NT, preferred_element_type=F32).astype(BF16)
    delta = heads.astype(F32) * saved[...].astype(F32)
    row_id = lax.broadcasted_iota(jnp.int32, (16, 128), 0)
    for a in range(PACK):
        at = slice(a * 128, a * 128 + 128)
        row = jnp.sum(jnp.transpose(delta[:, at]), axis=0, keepdims=True)
        stats = jnp.zeros((16, 128), F32)
        for i, piece in enumerate(pieces(logs[pl.ds(step * PACK + a, 1), :] * LOG2E) + pieces(row)):
            stats = jnp.where(row_id == i, piece, stats)
        packed[a, 0:128, :] = heads[:, at]
        packed[a, 128:144, :] = stats.astype(BF16)


PACK = 8
WHOLE = pl.BlockSpec((128, 2048), lambda h: (0, 0))
COLUMNS = pl.BlockSpec((128, 128 * PACK), lambda h: (0, h))


def pack_first(side, queries, keys, values, saved, cot):
    return pl.pallas_call(
        first_body,
        grid=(16 // PACK,),
        in_specs=[SMEM] + [COLUMNS] * 5,
        out_specs=[pl.BlockSpec((PACK, 384, 128), lambda h: (h, 0, 0))] + [WHOLE] * 4,
        out_shape=[like((16, 384, 128), BF16)] + [like((128, 2048), BF16)] * 4,
        compiler_params=pltpu.CompilerParams(vmem_limit_bytes=60 * 2**20),
        name="pack_first",
    )(side, queries, keys, values, saved, cot)


def pack_second(cot, weight, saved, logs):
    return pl.pallas_call(
        second_body,
        grid=(16 // PACK,),
        in_specs=[WHOLE, pl.BlockSpec((128 * PACK, 2048), lambda h: (h, 0)), COLUMNS,
                  pl.BlockSpec((16, 128), lambda h: (0, 0))],
        out_specs=pl.BlockSpec((PACK, 144, 128), lambda h: (h, 0, 0)),
        out_shape=like((16, 144, 128), BF16),
        compiler_params=pltpu.CompilerParams(vmem_limit_bytes=40 * 2**20),
        name="pack_second",
    )(cot, weight, saved, logs)


def sort_rows(rank, base, count, pairs):
    for j in range(count):
        at = pl.ds(pl.multiple_of(rank[base + j] * 64, 64), 64)
        for src, lo, dst in pairs:
            lo += (j % 2) * 64
            dst[at, :] = src[j // 2, lo : lo + 64, :]


def place_stats(q_rank, qd, stats_s):
    low = lax.broadcasted_iota(jnp.int32, (1, 128), 1) < 64
    for j in range(16):
        raw = qd[j, 128:144, :].astype(F32)
        for kind in range(2):
            row = raw[3 * kind : 3 * kind + 1] + raw[3 * kind + 1 : 3 * kind + 2] + raw[3 * kind + 2 : 3 * kind + 3]
            turned = pltpu.roll(row, 64, 1)
            for sub in range(2):
                r = q_rank[2 * j + sub]
                upper = r % 2
                value = jnp.where(upper == sub, row, turned)
                at = pl.ds(r // 2, 1)
                keep = jnp.logical_xor(low, upper == 1)
                stats_s[kind, at, :] = jnp.where(keep, value, stats_s[kind, at, :])


def tiles(plan, q_base, k_base, qs, dos, ks, vs, stats_s, dqs, dks, dvs, tq, tk, scaling, start, finish):
    n_q = qs.shape[0] // tq
    n_k = ks.shape[0] // tk
    lane = lax.broadcasted_iota(jnp.int32, (1, 128), 1)

    def k_step(i, _):
        k_at = pl.ds(pl.multiple_of(i * tk, tk), tk)
        start(i, k_at)

        def tile(j, masked, k_rows=tk, q_low=0):
            q_rows = tq - q_low
            q_at = pl.ds(pl.multiple_of(j * tq + q_low, 128), q_rows)
            k_at = pl.ds(pl.multiple_of(i * tk, tk), k_rows)
            first = j * (tq // 128) + q_low // 128
            spans = range(q_rows // 128)
            logs = jnp.concatenate([stats_s[0, pl.ds(first + a, 1), :] for a in spans], axis=1)
            delta = jnp.concatenate([stats_s[1, pl.ds(first + a, 1), :] for a in spans], axis=1)
            k = ks[k_at, :]
            q = qs[q_at, :]
            do = dos[q_at, :]
            s = lax.dot_general(k, q, NT, preferred_element_type=F32)
            p = jnp.exp2(s * (scaling * LOG2E) - logs)
            if masked:
                pos = []
                for a in spans:
                    b = (first + a) * 2
                    pos.append(jnp.where(lane < 64, q_base[b] * 64 + lane, q_base[b + 1] * 64 + lane - 64))
                pos = jnp.concatenate(pos, axis=1)
                parts = []
                for b in range(k_rows // 64):
                    at = k_base[i * (tk // 64) + b] * 64 + lax.broadcasted_iota(jnp.int32, (64, q_rows), 0)
                    parts.append(jnp.where(at <= pos, p[b * 64 : b * 64 + 64], 0.0))
                p = jnp.concatenate(parts, axis=0)
            dvs[k_at, :] += jnp.dot(p.astype(BF16), do, preferred_element_type=F32)
            dp = lax.dot_general(vs[k_at, :], do, NT, preferred_element_type=F32)
            ds = (p * (dp - delta)).astype(BF16)
            dks[k_at, :] += jnp.dot(ds, q, preferred_element_type=F32)
            dqs[q_at, :] += lax.dot_general(ds, k, TN, preferred_element_type=F32)
            return 0

        def edge(j, _):
            late = k_base[i * (tk // 64) + tk // 128] > q_base[(j + 1) * (tq // 64) - 1]
            early = q_base[j * (tq // 64) + tq // 128 - 1] < k_base[i * (tk // 64)]
            for short in (False, True):
                for high in (False, True):

                    @pl.when(jnp.logical_and(late == short, early == high))
                    def _():
                        tile(j, True, tk // 2 if short else tk, tq // 2 if high else 0)

            return 0

        lax.fori_loop(plan[0, i], plan[1, i], edge, 0)
        lax.fori_loop(plan[1, i], n_q, lambda j, c: tile(j, False), 0)
        finish(i, k_at)
        return 0

    lax.fori_loop(0, n_k, k_step, 0)


def near_body(plan, q_rank, q_base, k_rank, k_base, own, grads, kv_far, dq, dk_out, dv_out,
              qs, dos, ks, vs, stats_s, dqs, dks, dvs, sems, kv_s, fetch_sem, *, tq, tk, scaling):
    fetch = pltpu.make_async_copy(kv_far, kv_s, fetch_sem)
    fetch.start()
    sort_rows(q_rank, 0, 32, [(own, 0, qs), (grads, 0, dos)])
    sort_rows(k_rank, 0, 32, [(own, 128, ks), (own, 256, vs)])
    place_stats(q_rank, grads, stats_s)
    fetch.wait()
    sort_rows(k_rank, 32, 32, [(kv_s, 0, ks), (kv_s, 128, vs)])
    dqs[...] = jnp.zeros_like(dqs)

    def copies(i, k_at):
        return (
            pltpu.make_async_copy(dks.at[k_at, :], dk_out.at[k_at, :], sems.at[0, i]),
            pltpu.make_async_copy(dvs.at[k_at, :], dv_out.at[k_at, :], sems.at[1, i]),
        )

    def start(i, k_at):
        dks[k_at, :] = jnp.zeros((tk, 128), F32)
        dvs[k_at, :] = jnp.zeros((tk, 128), F32)

    def finish(i, k_at):
        for copy in copies(i, k_at):
            copy.start()

    tiles(plan, q_base, k_base, qs, dos, ks, vs, stats_s, dqs, dks, dvs, tq, tk, scaling, start, finish)
    for i in range(4096 // tk):
        for copy in copies(i, pl.ds(i * tk, tk)):
            copy.wait()
    for j in range(32):
        at = pl.ds(pl.multiple_of(q_rank[j] * 64, 64), 64)
        lo = (j % 2) * 64
        dq[j // 2, lo : lo + 64, :] = dqs[at, :] * scaling


def far_body(plan, q_rank, q_base, k_rank, k_base, own, kv_far, q_far, grads, dk_in, dv_in,
             dq_far, dk_own, dv_own, dkv_far,
             qs, dos, ks, vs, stats_s, dqs, dks, dvs, sems, kv_s, fetch_sem, *, tq, tk, scaling):
    def copies(i, k_at):
        return (
            pltpu.make_async_copy(dk_in.at[k_at, :], dks.at[k_at, :], sems.at[0, i]),
            pltpu.make_async_copy(dv_in.at[k_at, :], dvs.at[k_at, :], sems.at[1, i]),
        )

    for i in range(4096 // tk):
        for copy in copies(i, pl.ds(i * tk, tk)):
            copy.start()
    fetch = pltpu.make_async_copy(kv_far, kv_s, fetch_sem)
    fetch.start()
    sort_rows(q_rank, 0, 32, [(q_far, 0, qs), (grads, 0, dos)])
    sort_rows(k_rank, 0, 32, [(own, 128, ks), (own, 256, vs)])
    place_stats(q_rank, grads, stats_s)
    fetch.wait()
    sort_rows(k_rank, 32, 32, [(kv_s, 0, ks), (kv_s, 128, vs)])
    dqs[...] = jnp.zeros_like(dqs)

    def start(i, k_at):
        for copy in copies(i, k_at):
            copy.wait()

    def finish(i, k_at):
        pass

    tiles(plan, q_base, k_base, qs, dos, ks, vs, stats_s, dqs, dks, dvs, tq, tk, scaling, start, finish)
    for j in range(32):
        at = pl.ds(pl.multiple_of(q_rank[j] * 64, 64), 64)
        own_at = pl.ds(pl.multiple_of(k_rank[j] * 64, 64), 64)
        far_at = pl.ds(pl.multiple_of(k_rank[32 + j] * 64, 64), 64)
        lo = (j % 2) * 64
        dq_far[j // 2, lo : lo + 64, :] = (dqs[at, :] * scaling).astype(BF16)
        dk_own[j // 2, lo : lo + 64, :] = dks[own_at, :] * scaling
        dv_own[j // 2, lo : lo + 64, :] = dvs[own_at, :]
        dkv_far[j // 2, lo : lo + 64, :] = (dks[far_at, :] * scaling).astype(BF16)
        dkv_far[j // 2, 128 + lo : 192 + lo, :] = dvs[far_at, :].astype(BF16)


COST = pl.CostEstimate(flops=7 * 10**9, bytes_accessed=12 * 2**20, transcendentals=10**7)
SORTED = [pltpu.VMEM((2048, 128), BF16)] * 2 + [pltpu.VMEM((4096, 128), BF16)] * 2
SORTED += [pltpu.VMEM((2, 16, 128), F32), pltpu.VMEM((2048, 128), F32)]
FETCH = [pltpu.VMEM((16, 256, 128), BF16), pltpu.SemaphoreType.DMA]
TOTALS = [pltpu.VMEM((4096, 128), F32)] * 2


def in_hbm(array):
    return pltpu.with_memory_space_constraint(array, pltpu.HBM)


def attn_near(tables, own, grads, kv_far, tq, tk, scaling):
    return pl.pallas_call(
        functools.partial(near_body, tq=tq, tk=tk, scaling=scaling),
        in_specs=[SMEM] * 5 + [VMEM] * 2 + [HBM],
        out_specs=[VMEM, HBM, HBM],
        out_shape=[like((16, 128, 128), F32)] + [pltpu.HBM((4096, 128), F32)] * 2,
        scratch_shapes=SORTED + TOTALS + [pltpu.SemaphoreType.DMA((2, 4096 // tk))] + FETCH,
        compiler_params=pltpu.CompilerParams(vmem_limit_bytes=28 * 2**20),
        cost_estimate=COST,
        name="attn_near",
    )(*tables, own, grads, in_hbm(kv_far))


def attn_far(tables, own, kv_far, q_far, grads, dk_in, dv_in, tq, tk, scaling):
    return pl.pallas_call(
        functools.partial(far_body, tq=tq, tk=tk, scaling=scaling),
        in_specs=[SMEM] * 5 + [VMEM, HBM, VMEM, VMEM] + [HBM] * 2,
        out_specs=[VMEM] * 4,
        out_shape=[like((16, 128, 128), BF16), like((16, 128, 128), F32), like((16, 128, 128), F32),
                   like((16, 256, 128), BF16)],
        scratch_shapes=SORTED + TOTALS + [pltpu.SemaphoreType.DMA((2, 4096 // tk))] + FETCH,
        compiler_params=pltpu.CompilerParams(vmem_limit_bytes=28 * 2**20),
        cost_estimate=COST,
        name="attn_far",
    )(*tables, own, in_hbm(kv_far), q_far, grads, in_hbm(dk_in), in_hbm(dv_in))


def ranked(blocks):
    rank = jnp.sum((blocks[:, None] > blocks[None, :]).astype(jnp.int32), axis=1)
    hot = rank[None, :] == jnp.arange(blocks.shape[0], dtype=jnp.int32)[:, None]
    return rank, jnp.sum(jnp.where(hot, blocks[None, :], 0), axis=1)


def make_plan(q_sorted, k_sorted, tq, tk):
    q_max = q_sorted[tq // 64 - 1 :: tq // 64]
    q_min = q_sorted[:: tq // 64]
    k_min = k_sorted[:: tk // 64]
    k_max = k_sorted[tk // 64 - 1 :: tk // 64]
    first = jnp.sum((q_max[None, :] < k_min[:, None]).astype(jnp.int32), axis=1)
    whole = jnp.sum((q_min[None, :] <= k_max[:, None]).astype(jnp.int32), axis=1)
    return jnp.stack([first, jnp.maximum(first, whole)])


def weight_body(side, part0, part1, part2, part3, kept, given, total):
    parts = [part[...] for part in (part0, part1, part2, part3)]
    rows = jnp.concatenate([part[:, :1024] for part in parts], axis=0)
    cols = jnp.concatenate([part[:, 1024:] for part in parts], axis=0)
    total[...] = lax.dot_general(rows, cols, TN, preferred_element_type=F32)
    c = side[0]
    for block in range(16):
        mine = pl.ds(pl.multiple_of((block * 2 + c) * 32, 32), 32)
        other = pl.ds(pl.multiple_of((block * 2 + 1 - c) * 32, 32), 32)
        kept[block, :, :] = total[mine, :]
        given[block, :, :] = total[other, :].astype(BF16)


def weight_block(side, parts):
    return pl.pallas_call(
        weight_body,
        grid=(1,),
        in_specs=[SMEM] + [pl.BlockSpec((128, 2048), lambda i: (0, 0))] * 4,
        out_specs=[pl.BlockSpec((16, 32, 1024), lambda i: (0, 0, 0))] * 2,
        out_shape=[pltpu.HBM((16, 32, 1024), F32), like((16, 32, 1024), BF16)],
        scratch_shapes=[pltpu.VMEM((1024, 1024), F32)],
        compiler_params=pltpu.CompilerParams(vmem_limit_bytes=28 * 2**20),
        cost_estimate=pl.CostEstimate(flops=2 * 10**9, bytes_accessed=6 * 2**20, transcendentals=0),
        name="weight_block",
    )(side, *parts)


SEQ = ("z", "x", "y", "c")
TQ, TK = 512, 1024


def ring(array, axis, by):
    count = lax.axis_size(axis)
    return lax.ppermute(array, axis, [(i, (i + by) % count) for i in range(count)])


def pick(array, index, axis):
    return lax.dynamic_index_in_dim(array, index, axis, keepdims=False)


def by_token(array):
    return jnp.transpose(array, (1, 0, 2)).reshape(1, 128, 2048)


def step(block_pos, queries, keys, values, attn_out, log_sums, grad_out, out_weight):
    z, c, d = lax.axis_index("z"), lax.axis_index("c"), lax.axis_index("d")
    scaling = 128**-0.5
    packed, *parts = pack_first((z * 2 + d).reshape(1), queries[0], keys[0], values[0], attn_out[0], grad_out[0])
    own = lax.all_to_all(packed, ("x", "y"), 0, 0, tiled=True)
    parts = parts[:1] + [ring(parts[s], ("z", "d"), s) for s in range(1, 4)]
    packed = pack_second(grad_out[0], out_weight, attn_out[0], log_sums[0])
    grads = lax.all_to_all(packed, ("x", "y"), 0, 0, tiled=True)

    where = block_pos[0].reshape(2, 16, 2, 2)
    q_blocks = pick(where, c, 2)
    k_blocks = pick(where, z, 0)
    k_blocks = jnp.concatenate([pick(k_blocks, c, 1).reshape(-1), pick(k_blocks, 1 - c, 1).reshape(-1)])
    k_rank, k_sorted = ranked(k_blocks)
    tables = []
    for side in (z, 1 - z):
        q_rank, q_sorted = ranked(pick(q_blocks, side, 0).reshape(-1))
        tables.append((make_plan(q_sorted, k_sorted, TQ, TK), q_rank, q_sorted, k_rank, k_sorted))

    kept, given = weight_block(c.reshape(1), parts)
    given = ring(given, "c", 1)
    grads, tables = lax.optimization_barrier((grads, tables))
    kv_far = ring(own[:, 128:], "c", 1)
    q_far = ring(own[:, :128], "z", 1)
    grads_far = ring(grads, "z", 1)
    dq_near, dk_near, dv_near = attn_near(tables[0], own, grads, kv_far, TQ, TK, scaling)
    dk_near, kept, given = lax.optimization_barrier((dk_near, kept, given))
    blocks = (kept + given.astype(F32)).astype(BF16)
    blocks = lax.all_to_all(blocks, ("x", "y"), 0, 0, tiled=True)
    dq_far, dk_own, dv_own, dkv_far = attn_far(
        tables[1], own, kv_far, q_far, grads_far, dk_near, dv_near, TQ, TK, scaling
    )
    dkv_got = ring(dkv_far, "c", 1).astype(F32)
    dq_got = ring(dq_far, "z", 1)
    dkv = jnp.concatenate(
        [(dk_own + dkv_got[:, :128]).astype(BF16), (dv_own + dkv_got[:, 128:]).astype(BF16)], axis=1
    )
    dkv_out = lax.all_to_all(dkv, ("x", "y"), 0, 0, tiled=True)
    blocks, _ = lax.optimization_barrier((blocks, dkv))
    mine = jnp.sum(blocks.astype(F32), axis=0)
    other = ring(mine, "d", 1)
    weight = jnp.where(d == 0, jnp.concatenate([mine, other], axis=1), jnp.concatenate([other, mine], axis=1))

    dq_near, dq_got, _ = lax.optimization_barrier((dq_near, dq_got, dkv))
    dq = (dq_near + dq_got.astype(F32)).astype(BF16)
    dq, dkv_out = lax.optimization_barrier((dq, dkv_out))
    dq_out = lax.all_to_all(dq, ("x", "y"), 0, 0, tiled=True)
    return by_token(dq_out), by_token(dkv_out[:, :128]), by_token(dkv_out[:, 128:]), weight


def solution(mesh):
    split = Mesh(mesh.devices.reshape(2, 4, 4, 2, 2), ("z", "x", "y", "c", "d"))
    rows = P("d", SEQ, None)
    return jax.shard_map(
        step,
        mesh=split,
        in_specs=(P("d", None), rows, rows, rows, rows, P("d", None, SEQ), rows, P()),
        out_specs=(rows, rows, rows, P(SEQ, None)),
        check_vma=False,
    )
```

```python
import functools

import jax
import jax.numpy as jnp
from jax import lax
from jax.experimental import pallas as pl
from jax.experimental.pallas import tpu as pltpu
from jax.sharding import Mesh
from jax.sharding import PartitionSpec as P

F32, BF16 = jnp.float32, jnp.bfloat16
LOG2E = 1.4426950408889634
NT = (((1,), (1,)), ((), ()))
TN = (((0,), (0,)), ((), ()))
SMEM = pl.BlockSpec(memory_space=pltpu.SMEM)
VMEM = pl.BlockSpec(memory_space=pltpu.VMEM)
HBM = pl.BlockSpec(memory_space=pltpu.HBM)


def like(shape, dtype):
    return jax.ShapeDtypeStruct(shape, dtype)


def pieces(row):
    hi = row.astype(BF16).astype(F32)
    mid = (row - hi).astype(BF16).astype(F32)
    return [hi, mid, row - hi - mid]


def first_body(side, queries, keys, values, saved, cot, packed, part0, part1, part2, part3):
    step = pl.program_id(0)
    for a in range(PACK):
        at = slice(a * 128, a * 128 + 128)
        packed[a, 0:128, :] = queries[:, at]
        packed[a, 128:256, :] = keys[:, at]
        packed[a, 256:384, :] = values[:, at]
    for s, part in enumerate((part0, part1, part2, part3)):
        target = (side[0] + s) % 4

        @pl.when(target // 2 == step)
        def _():
            part[:, 0:1024] = saved[...]

        @pl.when(target % 2 == step)
        def _():
            part[:, 1024:2048] = cot[...]


def second_body(cot, weight, saved, logs, packed):
    step = pl.program_id(0)
    heads = lax.dot_general(cot[...], weight[...], NT, preferred_element_type=F32).astype(BF16)
    delta = heads.astype(F32) * saved[...].astype(F32)
    row_id = lax.broadcasted_iota(jnp.int32, (16, 128), 0)
    for a in range(PACK):
        at = slice(a * 128, a * 128 + 128)
        row = jnp.sum(jnp.transpose(delta[:, at]), axis=0, keepdims=True)
        stats = jnp.zeros((16, 128), F32)
        for i, piece in enumerate(pieces(logs[pl.ds(step * PACK + a, 1), :] * LOG2E) + pieces(row)):
            stats = jnp.where(row_id == i, piece, stats)
        packed[a, 0:128, :] = heads[:, at]
        packed[a, 128:144, :] = stats.astype(BF16)


PACK = 8
WHOLE = pl.BlockSpec((128, 2048), lambda h: (0, 0))
COLUMNS = pl.BlockSpec((128, 128 * PACK), lambda h: (0, h))


def pack_first(side, queries, keys, values, saved, cot):
    return pl.pallas_call(
        first_body,
        grid=(16 // PACK,),
        in_specs=[SMEM] + [COLUMNS] * 5,
        out_specs=[pl.BlockSpec((PACK, 384, 128), lambda h: (h, 0, 0))] + [WHOLE] * 4,
        out_shape=[like((16, 384, 128), BF16)] + [like((128, 2048), BF16)] * 4,
        compiler_params=pltpu.CompilerParams(vmem_limit_bytes=60 * 2**20),
        name="pack_first",
    )(side, queries, keys, values, saved, cot)


def pack_second(cot, weight, saved, logs):
    return pl.pallas_call(
        second_body,
        grid=(16 // PACK,),
        in_specs=[WHOLE, pl.BlockSpec((128 * PACK, 2048), lambda h: (h, 0)), COLUMNS,
                  pl.BlockSpec((16, 128), lambda h: (0, 0))],
        out_specs=pl.BlockSpec((PACK, 144, 128), lambda h: (h, 0, 0)),
        out_shape=like((16, 144, 128), BF16),
        compiler_params=pltpu.CompilerParams(vmem_limit_bytes=40 * 2**20),
        name="pack_second",
    )(cot, weight, saved, logs)


def sort_rows(rank, base, count, pairs):
    for j in range(count):
        at = pl.ds(pl.multiple_of(rank[base + j] * 64, 64), 64)
        for src, lo, dst in pairs:
            lo += (j % 2) * 64
            dst[at, :] = src[j // 2, lo : lo + 64, :]


def place_stats(q_rank, qd, stats_s):
    low = lax.broadcasted_iota(jnp.int32, (1, 128), 1) < 64
    for j in range(16):
        raw = qd[j, 128:144, :].astype(F32)
        for kind in range(2):
            row = raw[3 * kind : 3 * kind + 1] + raw[3 * kind + 1 : 3 * kind + 2] + raw[3 * kind + 2 : 3 * kind + 3]
            turned = pltpu.roll(row, 64, 1)
            for sub in range(2):
                r = q_rank[2 * j + sub]
                upper = r % 2
                value = jnp.where(upper == sub, row, turned)
                at = pl.ds(r // 2, 1)
                keep = jnp.logical_xor(low, upper == 1)
                stats_s[kind, at, :] = jnp.where(keep, value, stats_s[kind, at, :])


def tiles(plan, q_base, k_base, qs, dos, ks, vs, stats_s, dqs, dks, dvs, tq, tk, scaling, start, finish):
    n_q = qs.shape[0] // tq
    n_k = ks.shape[0] // tk
    lane = lax.broadcasted_iota(jnp.int32, (1, 128), 1)

    def k_step(i, _):
        k_at = pl.ds(pl.multiple_of(i * tk, tk), tk)
        start(i, k_at)

        def tile(j, masked, k_rows=tk, q_low=0):
            q_rows = tq - q_low
            q_at = pl.ds(pl.multiple_of(j * tq + q_low, 128), q_rows)
            k_at = pl.ds(pl.multiple_of(i * tk, tk), k_rows)
            first = j * (tq // 128) + q_low // 128
            spans = range(q_rows // 128)
            logs = jnp.concatenate([stats_s[0, pl.ds(first + a, 1), :] for a in spans], axis=1)
            delta = jnp.concatenate([stats_s[1, pl.ds(first + a, 1), :] for a in spans], axis=1)
            k = ks[k_at, :]
            q = qs[q_at, :]
            do = dos[q_at, :]
            s = lax.dot_general(k, q, NT, preferred_element_type=F32)
            p = jnp.exp2(s * (scaling * LOG2E) - logs)
            if masked:
                pos = []
                for a in spans:
                    b = (first + a) * 2
                    pos.append(jnp.where(lane < 64, q_base[b] * 64 + lane, q_base[b + 1] * 64 + lane - 64))
                pos = jnp.concatenate(pos, axis=1)
                parts = []
                for b in range(k_rows // 64):
                    at = k_base[i * (tk // 64) + b] * 64 + lax.broadcasted_iota(jnp.int32, (64, q_rows), 0)
                    parts.append(jnp.where(at <= pos, p[b * 64 : b * 64 + 64], 0.0))
                p = jnp.concatenate(parts, axis=0)
            dvs[k_at, :] += jnp.dot(p.astype(BF16), do, preferred_element_type=F32)
            dp = lax.dot_general(vs[k_at, :], do, NT, preferred_element_type=F32)
            ds = (p * (dp - delta)).astype(BF16)
            dks[k_at, :] += jnp.dot(ds, q, preferred_element_type=F32)
            dqs[q_at, :] += lax.dot_general(ds, k, TN, preferred_element_type=F32)
            return 0

        def edge(j, _):
            late = k_base[i * (tk // 64) + tk // 128] > q_base[(j + 1) * (tq // 64) - 1]
            early = q_base[j * (tq // 64) + tq // 128 - 1] < k_base[i * (tk // 64)]
            for short in (False, True):
                for high in (False, True):

                    @pl.when(jnp.logical_and(late == short, early == high))
                    def _():
                        tile(j, True, tk // 2 if short else tk, tq // 2 if high else 0)

            return 0

        lax.fori_loop(plan[0, i], plan[1, i], edge, 0)
        lax.fori_loop(plan[1, i], n_q, lambda j, c: tile(j, False), 0)
        finish(i, k_at)
        return 0

    lax.fori_loop(0, n_k, k_step, 0)


def near_body(plan, q_rank, q_base, k_rank, k_base, own, grads, kv_far, dq, dk_out, dv_out,
              qs, dos, ks, vs, stats_s, dqs, dks, dvs, sems, kv_s, fetch_sem, *, tq, tk, scaling):
    fetch = pltpu.make_async_copy(kv_far, kv_s, fetch_sem)
    fetch.start()
    sort_rows(q_rank, 0, 32, [(own, 0, qs), (grads, 0, dos)])
    sort_rows(k_rank, 0, 32, [(own, 128, ks), (own, 256, vs)])
    place_stats(q_rank, grads, stats_s)
    fetch.wait()
    sort_rows(k_rank, 32, 32, [(kv_s, 0, ks), (kv_s, 128, vs)])
    dqs[...] = jnp.zeros_like(dqs)

    def copies(i, k_at):
        return (
            pltpu.make_async_copy(dks.at[k_at, :], dk_out.at[k_at, :], sems.at[0, i]),
            pltpu.make_async_copy(dvs.at[k_at, :], dv_out.at[k_at, :], sems.at[1, i]),
        )

    def start(i, k_at):
        dks[k_at, :] = jnp.zeros((tk, 128), F32)
        dvs[k_at, :] = jnp.zeros((tk, 128), F32)

    def finish(i, k_at):
        for copy in copies(i, k_at):
            copy.start()

    tiles(plan, q_base, k_base, qs, dos, ks, vs, stats_s, dqs, dks, dvs, tq, tk, scaling, start, finish)
    for i in range(4096 // tk):
        for copy in copies(i, pl.ds(i * tk, tk)):
            copy.wait()
    for j in range(32):
        at = pl.ds(pl.multiple_of(q_rank[j] * 64, 64), 64)
        lo = (j % 2) * 64
        dq[j // 2, lo : lo + 64, :] = dqs[at, :] * scaling


def far_body(plan, q_rank, q_base, k_rank, k_base, own, kv_far, q_far, grads, dk_in, dv_in,
             dq_far, dk_own, dv_own, dkv_far,
             qs, dos, ks, vs, stats_s, dqs, dks, dvs, sems, kv_s, fetch_sem, *, tq, tk, scaling):
    def copies(i, k_at):
        return (
            pltpu.make_async_copy(dk_in.at[k_at, :], dks.at[k_at, :], sems.at[0, i]),
            pltpu.make_async_copy(dv_in.at[k_at, :], dvs.at[k_at, :], sems.at[1, i]),
        )

    for i in range(4096 // tk):
        for copy in copies(i, pl.ds(i * tk, tk)):
            copy.start()
    fetch = pltpu.make_async_copy(kv_far, kv_s, fetch_sem)
    fetch.start()
    sort_rows(q_rank, 0, 32, [(q_far, 0, qs), (grads, 0, dos)])
    sort_rows(k_rank, 0, 32, [(own, 128, ks), (own, 256, vs)])
    place_stats(q_rank, grads, stats_s)
    fetch.wait()
    sort_rows(k_rank, 32, 32, [(kv_s, 0, ks), (kv_s, 128, vs)])
    dqs[...] = jnp.zeros_like(dqs)

    def start(i, k_at):
        for copy in copies(i, k_at):
            copy.wait()

    def finish(i, k_at):
        pass

    tiles(plan, q_base, k_base, qs, dos, ks, vs, stats_s, dqs, dks, dvs, tq, tk, scaling, start, finish)
    for j in range(32):
        at = pl.ds(pl.multiple_of(q_rank[j] * 64, 64), 64)
        own_at = pl.ds(pl.multiple_of(k_rank[j] * 64, 64), 64)
        far_at = pl.ds(pl.multiple_of(k_rank[32 + j] * 64, 64), 64)
        lo = (j % 2) * 64
        dq_far[j // 2, lo : lo + 64, :] = (dqs[at, :] * scaling).astype(BF16)
        dk_own[j // 2, lo : lo + 64, :] = dks[own_at, :] * scaling
        dv_own[j // 2, lo : lo + 64, :] = dvs[own_at, :]
        dkv_far[j // 2, lo : lo + 64, :] = (dks[far_at, :] * scaling).astype(BF16)
        dkv_far[j // 2, 128 + lo : 192 + lo, :] = dvs[far_at, :].astype(BF16)


COST = pl.CostEstimate(flops=7 * 10**9, bytes_accessed=12 * 2**20, transcendentals=10**7)
SORTED = [pltpu.VMEM((2048, 128), BF16)] * 2 + [pltpu.VMEM((4096, 128), BF16)] * 2
SORTED += [pltpu.VMEM((2, 16, 128), F32), pltpu.VMEM((2048, 128), F32)]
FETCH = [pltpu.VMEM((16, 256, 128), BF16), pltpu.SemaphoreType.DMA]
TOTALS = [pltpu.VMEM((4096, 128), F32)] * 2


def in_hbm(array):
    return pltpu.with_memory_space_constraint(array, pltpu.HBM)


def attn_near(tables, own, grads, kv_far, tq, tk, scaling):
    return pl.pallas_call(
        functools.partial(near_body, tq=tq, tk=tk, scaling=scaling),
        in_specs=[SMEM] * 5 + [VMEM] * 2 + [HBM],
        out_specs=[VMEM, HBM, HBM],
        out_shape=[like((16, 128, 128), F32)] + [pltpu.HBM((4096, 128), F32)] * 2,
        scratch_shapes=SORTED + TOTALS + [pltpu.SemaphoreType.DMA((2, 4096 // tk))] + FETCH,
        compiler_params=pltpu.CompilerParams(vmem_limit_bytes=28 * 2**20),
        cost_estimate=COST,
        name="attn_near",
    )(*tables, own, grads, in_hbm(kv_far))


def attn_far(tables, own, kv_far, q_far, grads, dk_in, dv_in, tq, tk, scaling):
    return pl.pallas_call(
        functools.partial(far_body, tq=tq, tk=tk, scaling=scaling),
        in_specs=[SMEM] * 5 + [VMEM, HBM, VMEM, VMEM] + [HBM] * 2,
        out_specs=[VMEM] * 4,
        out_shape=[like((16, 128, 128), BF16), like((16, 128, 128), F32), like((16, 128, 128), F32),
                   like((16, 256, 128), BF16)],
        scratch_shapes=SORTED + TOTALS + [pltpu.SemaphoreType.DMA((2, 4096 // tk))] + FETCH,
        compiler_params=pltpu.CompilerParams(vmem_limit_bytes=28 * 2**20),
        cost_estimate=COST,
        name="attn_far",
    )(*tables, own, in_hbm(kv_far), q_far, grads, in_hbm(dk_in), in_hbm(dv_in))


def ranked(blocks):
    rank = jnp.sum((blocks[:, None] > blocks[None, :]).astype(jnp.int32), axis=1)
    hot = rank[None, :] == jnp.arange(blocks.shape[0], dtype=jnp.int32)[:, None]
    return rank, jnp.sum(jnp.where(hot, blocks[None, :], 0), axis=1)


def make_plan(q_sorted, k_sorted, tq, tk):
    q_max = q_sorted[tq // 64 - 1 :: tq // 64]
    q_min = q_sorted[:: tq // 64]
    k_min = k_sorted[:: tk // 64]
    k_max = k_sorted[tk // 64 - 1 :: tk // 64]
    first = jnp.sum((q_max[None, :] < k_min[:, None]).astype(jnp.int32), axis=1)
    whole = jnp.sum((q_min[None, :] <= k_max[:, None]).astype(jnp.int32), axis=1)
    return jnp.stack([first, jnp.maximum(first, whole)])


def weight_body(side, part0, part1, part2, part3, kept, given, total):
    parts = [part[:, :1024] for part in (part0, part1, part2, part3)]
    rows = jnp.concatenate(parts, axis=0)
    span = pl.ds(pl.multiple_of(1024 + pl.program_id(0) * 512, 512), 512)
    cols = jnp.concatenate([part[:, span] for part in (part0, part1, part2, part3)], axis=0)
    total[...] = lax.dot_general(rows, cols, TN, preferred_element_type=F32)
    c = side[0]
    for block in range(16):
        mine = pl.ds(pl.multiple_of((block * 2 + c) * 32, 32), 32)
        other = pl.ds(pl.multiple_of((block * 2 + 1 - c) * 32, 32), 32)
        kept[block, :, :] = total[mine, :]
        given[block, :, :] = total[other, :].astype(BF16)


def weight_block(side, parts):
    return pl.pallas_call(
        weight_body,
        grid=(2,),
        in_specs=[SMEM] + [pl.BlockSpec((128, 2048), lambda i: (0, 0))] * 4,
        out_specs=[pl.BlockSpec((16, 32, 512), lambda i: (0, 0, i))] * 2,
        out_shape=[pltpu.HBM((16, 32, 1024), F32), like((16, 32, 1024), BF16)],
        scratch_shapes=[pltpu.VMEM((1024, 512), F32)],
        compiler_params=pltpu.CompilerParams(vmem_limit_bytes=28 * 2**20),
        cost_estimate=pl.CostEstimate(flops=2 * 10**9, bytes_accessed=6 * 2**20, transcendentals=0),
        name="weight_block",
    )(side, *parts)


SEQ = ("z", "x", "y", "c")
TQ, TK = 512, 1024


def ring(array, axis, by):
    count = lax.axis_size(axis)
    return lax.ppermute(array, axis, [(i, (i + by) % count) for i in range(count)])


def pick(array, index, axis):
    return lax.dynamic_index_in_dim(array, index, axis, keepdims=False)


def by_token(array):
    return jnp.transpose(array, (1, 0, 2)).reshape(1, 128, 2048)


def step(block_pos, queries, keys, values, attn_out, log_sums, grad_out, out_weight):
    z, c, d = lax.axis_index("z"), lax.axis_index("c"), lax.axis_index("d")
    scaling = 128**-0.5
    packed, *parts = pack_first((z * 2 + d).reshape(1), queries[0], keys[0], values[0], attn_out[0], grad_out[0])
    own = lax.all_to_all(packed, ("x", "y"), 0, 0, tiled=True)
    parts = parts[:1] + [ring(parts[s], ("z", "d"), s) for s in range(1, 4)]
    packed = pack_second(grad_out[0], out_weight, attn_out[0], log_sums[0])
    grads = lax.all_to_all(packed, ("x", "y"), 0, 0, tiled=True)

    where = block_pos[0].reshape(2, 16, 2, 2)
    q_blocks = pick(where, c, 2)
    k_blocks = pick(where, z, 0)
    k_blocks = jnp.concatenate([pick(k_blocks, c, 1).reshape(-1), pick(k_blocks, 1 - c, 1).reshape(-1)])
    k_rank, k_sorted = ranked(k_blocks)
    tables = []
    for side in (z, 1 - z):
        q_rank, q_sorted = ranked(pick(q_blocks, side, 0).reshape(-1))
        tables.append((make_plan(q_sorted, k_sorted, TQ, TK), q_rank, q_sorted, k_rank, k_sorted))

    kept, given = weight_block(c.reshape(1), parts)
    given = ring(given, "c", 1)
    grads, tables = lax.optimization_barrier((grads, tables))
    kv_far = ring(own[:, 128:], "c", 1)
    q_far = ring(own[:, :128], "z", 1)
    grads_far = ring(grads, "z", 1)
    dq_near, dk_near, dv_near = attn_near(tables[0], own, grads, kv_far, TQ, TK, scaling)
    dk_near, kept, given = lax.optimization_barrier((dk_near, kept, given))
    blocks = (kept + given.astype(F32)).astype(BF16)
    blocks = lax.all_to_all(blocks, ("x", "y"), 0, 0, tiled=True)
    dq_far, dk_own, dv_own, dkv_far = attn_far(
        tables[1], own, kv_far, q_far, grads_far, dk_near, dv_near, TQ, TK, scaling
    )
    dkv_got = ring(dkv_far, "c", 1).astype(F32)
    dq_got = ring(dq_far, "z", 1)
    dkv = jnp.concatenate(
        [(dk_own + dkv_got[:, :128]).astype(BF16), (dv_own + dkv_got[:, 128:]).astype(BF16)], axis=1
    )
    dkv_out = lax.all_to_all(dkv, ("x", "y"), 0, 0, tiled=True)
    blocks, _ = lax.optimization_barrier((blocks, dkv))
    mine = jnp.sum(blocks.astype(F32), axis=0)
    other = ring(mine, "d", 1)
    weight = jnp.where(d == 0, jnp.concatenate([mine, other], axis=1), jnp.concatenate([other, mine], axis=1))

    dq_near, dq_got, _ = lax.optimization_barrier((dq_near, dq_got, dkv))
    dq = (dq_near + dq_got.astype(F32)).astype(BF16)
    dq, dkv_out = lax.optimization_barrier((dq, dkv_out))
    dq_out = lax.all_to_all(dq, ("x", "y"), 0, 0, tiled=True)
    return by_token(dq_out), by_token(dkv_out[:, :128]), by_token(dkv_out[:, 128:]), weight


def solution(mesh):
    split = Mesh(mesh.devices.reshape(2, 4, 4, 2, 2), ("z", "x", "y", "c", "d"))
    rows = P("d", SEQ, None)
    return jax.shard_map(
        step,
        mesh=split,
        in_specs=(P("d", None), rows, rows, rows, rows, P("d", None, SEQ), rows, P()),
        out_specs=(rows, rows, rows, P(SEQ, None)),
        check_vma=False,
    )
```
